32 devices in a mesh: ex: 16 (over z, y, core), ta: 2 (over x).
Axes of the slice: x: 2, y: 2, z: 4, core: 2. Of those that a mesh axis runs over, the one named last changes fastest.
Arguments:
- slot_expert: int32 [48], replicated, may hold values from 0 to 31, as said below
- gate_train: bfloat16 [32, 4096, 1024], P('ex', 'ta'), may hold values from -0.09375 to 0.09375
- up_train: bfloat16 [32, 4096, 1024], P('ex', 'ta'), may hold values from -0.09375 to 0.09375
- down_train: bfloat16 [32, 1024, 4096], P('ex', None, 'ta'), may hold values from -0.1875 to 0.1875
- slot_tokens: bfloat16 [48, 128, 4096], P('ex', None, 'ta'), may hold values from -6 to 6
Outputs:
- gate_serve: bfloat16 [48, 1024, 4096], P('ex', 'ta')
- up_serve: bfloat16 [48, 1024, 4096], P('ex', 'ta')
- down_serve: bfloat16 [48, 4096, 1024], P('ex', None, 'ta')
- expert_out: bfloat16 [48, 128, 4096], P('ex', None, 'ta')
The draws below stay inside these ranges and needn't reach their ends.
Inputs may be any that keep to these rules, and one draw needn't show every extreme that they name: `slot_expert`: every expert 0 to 32-1 is named by at least one slot. The 3 slots of one index p of ex (slots p*3 to p*3+3-1) name experts from 3 different blocks of 2 experts (block q holds experts q*2 to q*2+2-1), so every block of experts gives every block of slots at most one expert, and exactly one for 3 blocks.
All inputs are finite; a program needn't handle non-finite values.
Results may differ from the reference program's by a relative error of at most 0.0015.
Values may be sent and summed in bfloat16 or wider, within the bound.
A program may use at most 192 MiB of HBM per device.

```python
import jax
import jax.numpy as jnp
from jax import lax

D = 4096
FF = 1024
EXP_DEV = 2
CAP = 128
EXPERTS = 32
SLOT_DEV = 3
SLOTS = 48


def draw_slot_expert(key, part):
    groups = EXPERTS // EXP_DEV
    key_offset, key_label, key_rotate, key_hot, key_rank = jax.random.split(key, 5)
    offsets = jax.random.permutation(key_offset, groups)[:SLOT_DEV]
    relabel = jax.random.permutation(key_label, groups)
    rotate = jax.random.randint(key_rotate, (groups,), 0, EXP_DEV)
    hot_local = jax.random.randint(key_hot, (groups,), 0, EXP_DEV)
    dest_row = jnp.arange(groups, dtype=jnp.int32)
    column = jnp.arange(SLOT_DEV, dtype=jnp.int32)
    src_pos = (dest_row[:, None] + offsets[None, :]) % groups
    source = relabel[src_pos]
    local_index = jnp.where(column[None, :] < EXP_DEV, (column[None, :] + rotate[source]) % EXP_DEV, hot_local[source])
    expert_ids = (source * EXP_DEV + local_index).astype(jnp.int32)
    inverse = jnp.argsort(relabel, stable=True)
    expert_ids = expert_ids[inverse]
    rank_keys = jax.random.randint(key_rank, (groups, SLOT_DEV), 0, 1 << 20) * SLOT_DEV + column[None, :]
    ordering = jnp.argsort(rank_keys, axis=1, stable=True)
    expert_ids = jnp.take_along_axis(expert_ids, ordering, axis=1)
    return expert_ids.reshape(-1).astype(jnp.int32)


def level_of(stream_key, extent, cuts, smallest, high):
    factor_of = 1.0
    for position, blocks in cuts:
        draws = jax.random.uniform(jax.random.fold_in(jax.random.fold_in(stream_key, 6), position), (blocks,), jnp.float32, smallest / len(cuts), high / len(cuts))
        factor_of = factor_of * jnp.repeat(jnp.exp(draws), extent[position] // blocks).reshape((-1,) + (1,) * (len(extent) - 1 - position))
    return factor_of


def noise(key, extent, spread, limit, cuts=(), kind=jnp.bfloat16):
    drawn = jax.random.normal(key, extent, jnp.float32) * spread
    if len(cuts) > 0:
        drawn = level_of(key, extent, cuts, -0.22, 0.18) * drawn
    return jnp.clip(drawn, min=-limit, max=limit).astype(kind)


def setup_inputs(seed: int = 0) -> dict:
    key_of = jax.random.split(jax.random.key(seed), 6)
    slot_expert = draw_slot_expert(jax.random.fold_in(key_of[5], 71), 0)
    gate_train = noise(key_of[1], (EXPERTS, D, FF), D ** -0.5, 0.09375, ((0, 16), (1, 2)))
    up_train = noise(key_of[2], (EXPERTS, D, FF), D ** -0.5, 0.09375, ((0, 16), (1, 2)))
    down_train = noise(key_of[3], (EXPERTS, FF, D), FF ** -0.5, 0.1875, ((0, 16), (2, 2)))
    slot_tokens = noise(key_of[4], (SLOTS, CAP, D), 1.0, 6.0, ((0, 16), (2, 2)))
    return dict(slot_expert=slot_expert, gate_train=gate_train, up_train=up_train, down_train=down_train, slot_tokens=slot_tokens)


def per_slot(operands):
    rows_in, gate_mat, up_mat, down_mat = operands
    gate_act = jnp.dot(rows_in, gate_mat.T, preferred_element_type=jnp.float32)
    up_act = jnp.dot(rows_in, up_mat.T, preferred_element_type=jnp.float32)
    hidden = (jax.nn.silu(gate_act) * up_act).astype(jnp.bfloat16)
    return jnp.dot(hidden, down_mat.T, preferred_element_type=jnp.float32).astype(jnp.bfloat16)


def reference(slot_expert, gate_train, up_train, down_train, slot_tokens):
    gate_serve = jnp.swapaxes(jnp.take(gate_train, slot_expert, axis=0), 1, 2)
    up_serve = jnp.swapaxes(jnp.take(up_train, slot_expert, axis=0), 1, 2)
    down_serve = jnp.swapaxes(jnp.take(down_train, slot_expert, axis=0), 1, 2)
    expert_out = lax.map(per_slot, (slot_tokens, gate_serve, up_serve, down_serve))
    return gate_serve, up_serve, down_serve, expert_out
```

```python
import jax
import jax.numpy as jnp
from jax import lax
from jax.sharding import PartitionSpec as P


def swap_over(x, axis, split, concat):
    size = lax.axis_size(axis)
    me = lax.axis_index(axis)
    width = x.shape[split] // size
    length = x.shape[concat]
    shape = list(x.shape)
    shape[split] = width
    shape[concat] = length * size
    out = jnp.zeros(shape, x.dtype)
    for shift in range(size):
        target = lax.rem(me + shift, size)
        source = lax.rem(me - shift + size, size)
        block = lax.dynamic_slice_in_dim(x, target * width, width, split)
        if shift:
            block = lax.ppermute(block, axis, [(i, (i + shift) % size) for i in range(size)])
        out = lax.dynamic_update_slice_in_dim(out, block, source * length, concat)
    return out


def spread(x):
    size = lax.axis_size("ex")
    local, rows, cols = x.shape
    parts = jnp.swapaxes(x.reshape(local, size, rows // size, cols), 0, 1)
    got = lax.all_to_all(parts, "ex", split_axis=0, concat_axis=0, tiled=True)
    return got.reshape(size * local, rows // size, cols)


def deliver(x, wanted):
    size = lax.axis_size("ex")
    rows, cols = x.shape[1:]
    packed = x.at[wanted].get(mode="promise_in_bounds")
    packed = packed.reshape(size, -1, rows, cols)
    got = lax.all_to_all(packed, "ex", split_axis=0, concat_axis=0, tiled=True)
    return jnp.swapaxes(got, 0, 1).reshape(-1, size * rows, cols)


def after(x, earlier):
    return lax.optimization_barrier((x, earlier))


def body(slot_expert, gate_train, up_train, down_train, slot_tokens):
    wanted = slot_expert.astype(jnp.int32)
    down_rows = jnp.swapaxes(down_train, 1, 2)
    gate_wide = swap_over(jnp.swapaxes(gate_train, 1, 2), "ta", 1, 2)
    up_wide = swap_over(jnp.swapaxes(up_train, 1, 2), "ta", 1, 2)
    tokens = lax.all_gather(slot_tokens, "ta", axis=2, tiled=True)

    down_spread = spread(down_rows)
    gate_wide, down_spread = after(gate_wide, down_spread)
    gate_spread = spread(gate_wide)
    up_wide, gate_spread = after(up_wide, gate_spread)
    up_spread = spread(up_wide)

    down_spread, up_spread = after(down_spread, up_spread)
    down_slots = deliver(down_spread, wanted)
    gate_spread, down_slots = after(gate_spread, down_slots)
    gate_serve = deliver(gate_spread, wanted)
    down_serve = swap_over(down_slots, "ta", 2, 1)
    up_spread, gate_serve = after(up_spread, gate_serve)
    up_serve = deliver(up_spread, wanted)

    gate_act = jnp.einsum("sck,sfk->scf", tokens, gate_serve, preferred_element_type=jnp.float32)
    up_act = jnp.einsum("sck,sfk->scf", tokens, up_serve, preferred_element_type=jnp.float32)
    hidden = (jax.nn.silu(gate_act) * up_act).astype(jnp.bfloat16)
    hidden = lax.all_gather(hidden, "ta", axis=2, tiled=True)
    expert_out = jnp.einsum(
        "scf,sdf->scd", hidden, down_slots, preferred_element_type=jnp.float32
    ).astype(jnp.bfloat16)
    return (gate_serve, up_serve, down_serve, expert_out)


def solution(mesh):
    placed = (
        P(),
        P("ex", "ta", None),
        P("ex", "ta", None),
        P("ex", None, "ta"),
        P("ex", None, "ta"),
    )
    return jax.shard_map(
        body,
        mesh=mesh,
        in_specs=placed,
        out_specs=(
            P("ex", "ta", None),
            P("ex", "ta", None),
            P("ex", None, "ta"),
            P("ex", None, "ta"),
        ),
        check_vma=False,
    )
```
